8 devices in a mesh: dp: 1 (over z), tp: 2 (over y), pp: 4 (over x, core).
Axes of the slice: x: 2, y: 2, z: 1, core: 2. Of those that a mesh axis runs over, the one named last changes fastest.
Arguments:
- x_in: bfloat16 [16, 4, 256, 1024], P('dp')
- g_out: float32 [16, 4, 256, 1024], P('dp')
- ln1_gain: float32 [4, 1024], P('pp')
- ln1_bias: float32 [4, 1024], P('pp')
- w_qkv: bfloat16 [4, 1024, 16, 3, 64], P('pp', None, 'tp')
- b_qkv: bfloat16 [4, 16, 3, 64], P('pp', 'tp')
- w_out: bfloat16 [4, 16, 64, 1024], P('pp', 'tp')
- b_out: bfloat16 [4, 1024], P('pp')
- ln2_gain: float32 [4, 1024], P('pp')
- ln2_bias: float32 [4, 1024], P('pp')
- w_up: bfloat16 [4, 1024, 4096], P('pp', None, 'tp')
- b_up: bfloat16 [4, 4096], P('pp', 'tp')
- w_down: bfloat16 [4, 4096, 1024], P('pp', 'tp')
- b_down: bfloat16 [4, 1024], P('pp')
Outputs:
- output 1: bfloat16 [16, 4, 256, 1024], P('dp')
- output 2: float32 [4, 1024], P(('dp', 'pp'))
- output 3: float32 [4, 1024], P(('dp', 'pp'))
- output 4: float32 [4, 1024, 16, 3, 64], P(('dp', 'pp'), None, 'tp')
- output 5: float32 [4, 16, 3, 64], P(('dp', 'pp'), 'tp')
- output 6: float32 [4, 16, 64, 1024], P(('dp', 'pp'), 'tp')
- output 7: float32 [4, 1024], P(('dp', 'pp'))
- output 8: float32 [4, 1024], P(('dp', 'pp'))
- output 9: float32 [4, 1024], P(('dp', 'pp'))
- output 10: float32 [4, 1024, 4096], P(('dp', 'pp'), None, 'tp')
- output 11: float32 [4, 4096], P(('dp', 'pp'), 'tp')
- output 12: float32 [4, 4096, 1024], P(('dp', 'pp'), 'tp')
- output 13: float32 [4, 1024], P(('dp', 'pp'))
All inputs are finite; a program needn't handle non-finite values.
Results may differ from the reference program's by a relative error of at most 0.0177431.
Values are sent between devices in bfloat16 or wider.
A program may use at most 1 GiB of HBM per device.

```python
import jax
import jax.numpy as jnp
from jax import lax

NUM_MICRO = 16
MICRO_ROWS = 4
SEQ_LEN = 256
MODEL_DIM = 1024
NUM_HEADS = 16
HEAD_DIM = 64
FFN_DIM = 4096
NUM_STAGES = 4
ROT_DIM = HEAD_DIM // 4


def norm_core(hidden, gain, shift):
    center = hidden - jnp.mean(hidden, axis=-1, keepdims=True)
    var_term = jnp.mean(center * center, axis=-1, keepdims=True)
    return center * lax.rsqrt(var_term + 1e-5) * gain + shift


def rotary_tables():
    half_rot = ROT_DIM // 2
    inv_freq = 10000.0 ** (-(jnp.arange(half_rot, dtype=jnp.float32) * 2.0) / ROT_DIM)
    angles = jnp.arange(SEQ_LEN, dtype=jnp.float32)[:, None] * inv_freq[None, :]
    angles = jnp.concatenate([angles, angles], axis=-1)
    return jnp.cos(angles)[None, :, None, :], jnp.sin(angles)[None, :, None, :]


def apply_rotary(values, cos_tab, sin_tab):
    half_rot = ROT_DIM // 2
    rot_part = values[..., :ROT_DIM]
    turned = jnp.concatenate([-rot_part[..., half_rot:], rot_part[..., :half_rot]], axis=-1)
    return jnp.concatenate([rot_part * cos_tab + turned * sin_tab, values[..., ROT_DIM:]], axis=-1)


def attention(qkv_proj, cos_tab, sin_tab):
    query = apply_rotary(qkv_proj[:, :, :, 0].astype(jnp.float32), cos_tab, sin_tab).astype(jnp.bfloat16)
    key_rot = apply_rotary(qkv_proj[:, :, :, 1].astype(jnp.float32), cos_tab, sin_tab).astype(jnp.bfloat16)
    value_part = qkv_proj[:, :, :, 2]
    scores = jnp.einsum('bqhe,bkhe->bhqk', query.astype(jnp.float32), key_rot.astype(jnp.float32)) * (HEAD_DIM ** -0.5)
    positions = jnp.arange(SEQ_LEN)
    causal = positions[:, None] >= positions[None, :]
    scores = jnp.where(causal, scores, -1e30)
    probs = jax.nn.softmax(scores, axis=-1).astype(jnp.bfloat16)
    context = jnp.einsum('bhqk,bkhe->bqhe', probs.astype(jnp.float32), value_part.astype(jnp.float32))
    return context.astype(jnp.bfloat16)


def layer_forward(hidden, layer_wts, cos_tab, sin_tab):
    ln1_gain, ln1_bias, w_qkv, b_qkv, w_out, b_out, ln2_gain, ln2_bias, w_up, b_up, w_down, b_down = layer_wts
    tokens = MICRO_ROWS * SEQ_LEN
    hidden_f = hidden.reshape(tokens, MODEL_DIM).astype(jnp.float32)
    normed_a = norm_core(hidden_f, ln1_gain, ln1_bias).astype(jnp.bfloat16)
    normed_m = norm_core(hidden_f, ln2_gain, ln2_bias).astype(jnp.bfloat16)
    qkv_proj = jnp.dot(normed_a, w_qkv.reshape(MODEL_DIM, 3 * MODEL_DIM), preferred_element_type=jnp.float32)
    qkv_proj = (qkv_proj + b_qkv.reshape(3 * MODEL_DIM).astype(jnp.float32)).astype(jnp.bfloat16)
    qkv_proj = qkv_proj.reshape(MICRO_ROWS, SEQ_LEN, NUM_HEADS, 3, HEAD_DIM)
    context = attention(qkv_proj, cos_tab, sin_tab).reshape(tokens, MODEL_DIM)
    attn_sum = jnp.dot(context, w_out.reshape(MODEL_DIM, MODEL_DIM), preferred_element_type=jnp.float32)
    pre_act = jnp.dot(normed_m, w_up, preferred_element_type=jnp.float32) + b_up.astype(jnp.float32)
    hidden_mlp = jax.nn.gelu(pre_act, approximate=False).astype(jnp.bfloat16)
    mlp_sum = jnp.dot(hidden_mlp, w_down, preferred_element_type=jnp.float32)
    total = hidden_f + attn_sum + b_out.astype(jnp.float32) + mlp_sum + b_down.astype(jnp.float32)
    return total.astype(jnp.bfloat16).reshape(MICRO_ROWS, SEQ_LEN, MODEL_DIM)


def setup_inputs(seed: int = 0, part: int = 0) -> dict:
    weight_keys = jax.random.split(jax.random.key(seed), 12)
    data_keys = jax.random.split(jax.random.fold_in(jax.random.key(seed + 1), part), 2)
    act_shape = (NUM_MICRO, MICRO_ROWS, SEQ_LEN, MODEL_DIM)
    tokens = NUM_MICRO * MICRO_ROWS * SEQ_LEN
    vec_shape = (NUM_STAGES, MODEL_DIM)
    x_in = jax.random.normal(data_keys[0], act_shape, jnp.float32).astype(jnp.bfloat16)
    g_out = jax.random.normal(data_keys[1], act_shape, jnp.float32) * (tokens ** -0.5)
    return {
        'x_in': x_in,
        'g_out': g_out,
        'ln1_gain': 1.0 + 0.3 * jax.random.normal(weight_keys[0], vec_shape, jnp.float32),
        'ln1_bias': 0.3 * jax.random.normal(weight_keys[1], vec_shape, jnp.float32),
        'w_qkv': (jax.random.normal(weight_keys[2], (NUM_STAGES, MODEL_DIM, NUM_HEADS, 3, HEAD_DIM), jnp.float32) * MODEL_DIM ** -0.5).astype(jnp.bfloat16),
        'b_qkv': (0.5 * jax.random.normal(weight_keys[3], (NUM_STAGES, NUM_HEADS, 3, HEAD_DIM), jnp.float32)).astype(jnp.bfloat16),
        'w_out': (jax.random.normal(weight_keys[4], (NUM_STAGES, NUM_HEADS, HEAD_DIM, MODEL_DIM), jnp.float32) * MODEL_DIM ** -0.5).astype(jnp.bfloat16),
        'b_out': (0.5 * jax.random.normal(weight_keys[5], vec_shape, jnp.float32)).astype(jnp.bfloat16),
        'ln2_gain': 1.0 + 0.3 * jax.random.normal(weight_keys[6], vec_shape, jnp.float32),
        'ln2_bias': 0.3 * jax.random.normal(weight_keys[7], vec_shape, jnp.float32),
        'w_up': (jax.random.normal(weight_keys[8], (NUM_STAGES, MODEL_DIM, FFN_DIM), jnp.float32) * MODEL_DIM ** -0.5).astype(jnp.bfloat16),
        'b_up': (0.5 * jax.random.normal(weight_keys[9], (NUM_STAGES, FFN_DIM), jnp.float32)).astype(jnp.bfloat16),
        'w_down': (jax.random.normal(weight_keys[10], (NUM_STAGES, FFN_DIM, MODEL_DIM), jnp.float32) * FFN_DIM ** -0.5).astype(jnp.bfloat16),
        'b_down': (0.5 * jax.random.normal(weight_keys[11], vec_shape, jnp.float32)).astype(jnp.bfloat16),
    }


def reference(x_in, g_out, ln1_gain, ln1_bias, w_qkv, b_qkv, w_out, b_out, ln2_gain, ln2_bias, w_up, b_up, w_down, b_down):
    params = (ln1_gain, ln1_bias, w_qkv, b_qkv, w_out, b_out, ln2_gain, ln2_bias, w_up, b_up, w_down, b_down)
    cos_tab, sin_tab = rotary_tables()

    def layer_step(hidden, layer_wts):
        return layer_forward(hidden, layer_wts, cos_tab, sin_tab), None

    def stack_forward(layer_stack, hidden):
        final, unused = lax.scan(jax.checkpoint(layer_step), hidden, layer_stack)
        return final

    def micro_step(grad_acc, micro_pair):
        x_micro, g_micro = micro_pair
        y_micro, pullback = jax.vjp(lambda layer_stack: stack_forward(layer_stack, x_micro), params)
        (grads,) = pullback(g_micro.astype(jnp.bfloat16))
        grad_acc = jax.tree.map(lambda running, update: running + update.astype(jnp.float32), grad_acc, grads)
        return grad_acc, y_micro

    zeros = jax.tree.map(lambda weight: jnp.zeros(weight.shape, jnp.float32), params)
    grad_sum, y_all = lax.scan(micro_step, zeros, (x_in, g_out))
    return (y_all, grad_sum[0], grad_sum[1], grad_sum[2], grad_sum[3], grad_sum[4], grad_sum[5], grad_sum[6], grad_sum[7], grad_sum[8], grad_sum[9], grad_sum[10], grad_sum[11])
```

```python
import jax
import jax.numpy as jnp
from jax import lax
from jax.experimental import pallas as pl
from jax.experimental.pallas import tpu as pltpu
from jax.sharding import PartitionSpec as P

ROPE_BASE = 10000.0
LN_EPS = 1e-5
HEAD_DIM = 64
STAGE_SPECS = (P('pp', None), P('pp', None), P('pp', None, 'tp', None, None), P('pp', 'tp', None, None), P('pp', 'tp', None, None), P('pp', None), P('pp', None), P('pp', None), P('pp', None, 'tp'), P('pp', 'tp'), P('pp', 'tp', None), P('pp', None))
GRAD_SPECS = (P(('dp', 'pp'), None), P(('dp', 'pp'), None), P(('dp', 'pp'), None, 'tp', None, None), P(('dp', 'pp'), 'tp', None, None), P(('dp', 'pp'), 'tp', None, None), P(('dp', 'pp'), None), P(('dp', 'pp'), None), P(('dp', 'pp'), None), P(('dp', 'pp'), None, 'tp'), P(('dp', 'pp'), 'tp'), P(('dp', 'pp'), 'tp', None), P(('dp', 'pp'), None))
F32 = jnp.float32
BF16 = jnp.bfloat16
NN = (((1,), (0,)), ((), ()))
NT = (((1,), (1,)), ((), ()))
TN = (((0,), (0,)), ((), ()))


def dot(lhs, rhs, dims):
    return lax.dot_general(lhs, rhs, dims, preferred_element_type=F32)


def rotary_lanes(seq_len):
    rot_dim = HEAD_DIM // 4
    half_rot = rot_dim // 2
    inv_freq = ROPE_BASE ** (-(jnp.arange(half_rot, dtype=F32) * 2.0) / rot_dim)
    angles = jnp.arange(seq_len, dtype=F32)[:, None] * inv_freq[None, :]
    cos, sin = jnp.cos(angles), jnp.sin(angles)
    rest = HEAD_DIM - rot_dim
    zero_half, zero_rest = jnp.zeros_like(sin), jnp.zeros((seq_len, rest), F32)
    own = jnp.concatenate([cos, cos, jnp.ones((seq_len, rest), F32)], axis=1)
    above = jnp.concatenate([-sin, zero_half, zero_rest], axis=1)
    below = jnp.concatenate([zero_half, sin, zero_rest], axis=1)
    return jnp.stack([jnp.tile(tab, (1, 2)) for tab in (own, above, below)])


def rotate(values, tabs):
    return values * tabs[0] + pltpu.roll(values, 120, 1) * tabs[1] + pltpu.roll(values, 8, 1) * tabs[2]


def rotate_back(values, tabs):
    return values * tabs[0] + pltpu.roll(values * tabs[1], 8, 1) + pltpu.roll(values * tabs[2], 120, 1)


def pair_columns(pair, half_cols):
    pairs_per_half = half_cols // 3 // 128
    base = (pair // pairs_per_half) * half_cols + (pair % pairs_per_half) * 128
    return [pl.ds(pl.multiple_of(base + part * (half_cols // 3), 128), 128) for part in range(3)]


def softmax_rows(query, key, causal):
    scores = dot(query, key, NT) * (HEAD_DIM ** -0.5)
    scores = jnp.where(causal, scores, -1e30)
    expo = jnp.exp(scores - jnp.max(scores, axis=1, keepdims=True))
    return expo / jnp.sum(expo, axis=1, keepdims=True)


def attention_forward_kernel(tabs_ref, qkv_ref, ctx_ref):
    seq_len = qkv_ref.shape[0]
    half_cols = qkv_ref.shape[1] // 2
    causal = lax.broadcasted_iota(jnp.int32, (seq_len, seq_len), 0) >= lax.broadcasted_iota(jnp.int32, (seq_len, seq_len), 1)
    first = lax.broadcasted_iota(jnp.int32, (seq_len, 128), 1) < HEAD_DIM
    tabs = (tabs_ref[0], tabs_ref[1], tabs_ref[2])

    @pl.loop(0, ctx_ref.shape[1] // 128, unroll=2)
    def pair_step(pair):
        q_col, k_col, v_col = pair_columns(pair, half_cols)
        query = rotate(qkv_ref[:, q_col].astype(F32), tabs)
        key = rotate(qkv_ref[:, k_col].astype(F32), tabs).astype(BF16)
        value = qkv_ref[:, v_col]
        outs = []
        for keep in (first, ~first):
            probs = softmax_rows(jnp.where(keep, query, 0.0).astype(BF16), key, causal).astype(BF16)
            outs.append(dot(probs, value, NN))
        ctx_ref[:, pl.ds(pl.multiple_of(pair * 128, 128), 128)] = jnp.where(first, outs[0], outs[1]).astype(BF16)


def attention_backward_kernel(tabs_ref, qkv_ref, gctx_ref, gqkv_ref):
    seq_len = qkv_ref.shape[0]
    half_cols = qkv_ref.shape[1] // 2
    causal = lax.broadcasted_iota(jnp.int32, (seq_len, seq_len), 0) >= lax.broadcasted_iota(jnp.int32, (seq_len, seq_len), 1)
    first = lax.broadcasted_iota(jnp.int32, (seq_len, 128), 1) < HEAD_DIM
    tabs = (tabs_ref[0], tabs_ref[1], tabs_ref[2])

    @pl.loop(0, gctx_ref.shape[1] // 128)
    def pair_step(pair):
        q_col, k_col, v_col = pair_columns(pair, half_cols)
        query32 = rotate(qkv_ref[:, q_col].astype(F32), tabs)
        query = query32.astype(BF16)
        key = rotate(qkv_ref[:, k_col].astype(F32), tabs).astype(BF16)
        value = qkv_ref[:, v_col]
        gctx = gctx_ref[:, pl.ds(pl.multiple_of(pair * 128, 128), 128)]
        gctx32 = gctx.astype(F32)
        parts = []
        for keep in (first, ~first):
            probs = softmax_rows(jnp.where(keep, query32, 0.0).astype(BF16), key, causal)
            gprobs = dot(jnp.where(keep, gctx32, 0.0).astype(BF16), value, NT)
            gvalue = dot(probs.astype(BF16), gctx, TN)
            gscores = probs * (gprobs - jnp.sum(gprobs * probs, axis=1, keepdims=True))
            gscores = (gscores * (HEAD_DIM ** -0.5)).astype(BF16)
            parts.append((dot(gscores, key, NN), dot(gscores, query, TN), gvalue))
        gquery, gkey, gvalue = (jnp.where(first, one, two) for one, two in zip(*parts))
        gqkv_ref[:, q_col] = rotate_back(gquery, tabs).astype(BF16)
        gqkv_ref[:, k_col] = rotate_back(gkey, tabs).astype(BF16)
        gqkv_ref[:, v_col] = gvalue.astype(BF16)


def attention_call(kernel, tabs, seq_len, out_cols, n_dots, *arrays):
    tokens = arrays[0].shape[0]
    rows = tokens // seq_len
    width = arrays[0].shape[1] // 3
    heads = width // HEAD_DIM
    return pl.pallas_call(
        kernel,
        grid=(rows,),
        in_specs=[pl.BlockSpec(tabs.shape, lambda i: (0, 0, 0))] + [pl.BlockSpec((seq_len, array.shape[1]), lambda i: (i, 0)) for array in arrays],
        out_specs=pl.BlockSpec((seq_len, out_cols), lambda i: (i, 0)),
        out_shape=jax.ShapeDtypeStruct((tokens, out_cols), BF16),
        compiler_params=pltpu.CompilerParams(dimension_semantics=('arbitrary',), vmem_limit_bytes=48 * 1024 * 1024),
        cost_estimate=pl.CostEstimate(flops=2 * n_dots * rows * heads * seq_len * seq_len * 256, bytes_accessed=2 * tokens * (sum(a.shape[1] for a in arrays) + out_cols), transcendentals=rows * heads * seq_len * seq_len),
    )(tabs, *arrays)


def normalize(hidden):
    hidden_f = hidden.astype(F32)
    center = hidden_f - jnp.mean(hidden_f, axis=-1, keepdims=True)
    inv_std = lax.rsqrt(jnp.mean(center * center, axis=-1, keepdims=True) + LN_EPS)
    return center * inv_std, inv_std


def gelu_parts(pre_act):
    cdf = 0.5 * (1.0 + lax.erf(pre_act * (2.0 ** -0.5)))
    return cdf


def solution(mesh):
    everyone = ('pp', 'tp')

    def device_fn(x_in, g_out, ln1_gain, ln1_bias, w_qkv, b_qkv, w_out, b_out, ln2_gain, ln2_bias, w_up, b_up, w_down, b_down):
        n_stages, tp_size = mesh.shape['pp'], mesh.shape['tp']
        n_dev = n_stages * tp_size
        stage_id = lax.axis_index('pp')
        rank = stage_id * tp_size + lax.axis_index('tp')
        n_micro, n_rows, seq_len, width = x_in.shape
        own_micro = n_micro // n_dev
        tokens = own_micro * n_rows * seq_len
        tabs = rotary_lanes(seq_len)

        def gather(shard):
            return lax.all_gather(shard, everyone, axis=0, tiled=True)

        heads = w_qkv.shape[2]
        qkv_shard = jnp.transpose(w_qkv[0], (2, 1, 3, 0)).reshape(3 * heads * HEAD_DIM, width)
        up_shard = jnp.transpose(w_up[0])
        out_shard = w_out[0].reshape(heads * HEAD_DIM, width)
        all_qkv = gather(qkv_shard)
        all_out = gather(out_shard)
        all_up = gather(up_shard)
        all_down = gather(w_down[0])

        def small(own, columns):
            return own.reshape(1, columns).astype(F32)

        b_qkv_own = jnp.transpose(b_qkv[0], (1, 0, 2)).reshape(1, -1)
        vec_own = jnp.concatenate([small(b_qkv_own, 3 * heads * HEAD_DIM), small(b_up, b_up.shape[1]), ln1_gain, ln1_bias, ln2_gain, ln2_bias, small(b_out, width), small(b_down, width)], axis=1)
        vec_all = gather(vec_own).reshape(n_stages, tp_size, -1)
        cut = 0

        def take(columns, split):
            nonlocal cut
            part = vec_all[:, :, cut:cut + columns] if split else vec_all[:, 0, cut:cut + columns]
            cut += columns
            return part.reshape(n_stages, -1)

        bias_qkv = take(3 * heads * HEAD_DIM, True)
        bias_up = take(b_up.shape[1], True)
        gain1, shift1, gain2, shift2, bias_out, bias_down = (take(width, False) for _ in range(6))

        def layer(stack, index):
            rows = stack.shape[0] // n_stages
            return stack[index * rows:(index + 1) * rows]

        x_own = lax.dynamic_slice_in_dim(x_in, rank * own_micro, own_micro, 0).reshape(tokens, width)
        g_own = lax.dynamic_slice_in_dim(g_out, rank * own_micro, own_micro, 0).reshape(tokens, width).astype(BF16)

        hidden = x_own
        saved = []
        for index in range(n_stages):
            normed, _ = normalize(hidden)
            normed_a = (normed * gain1[index] + shift1[index]).astype(BF16)
            normed_m = (normed * gain2[index] + shift2[index]).astype(BF16)
            qkv_proj = (dot(normed_a, layer(all_qkv, index), NT) + bias_qkv[index]).astype(BF16)
            context = attention_call(attention_forward_kernel, tabs, seq_len, width, 2, qkv_proj)
            pre_act = dot(normed_m, layer(all_up, index), NT) + bias_up[index]
            hidden_mlp = (pre_act * gelu_parts(pre_act)).astype(BF16)
            attn_sum = dot(context, layer(all_out, index), NN)
            mlp_sum = dot(hidden_mlp, layer(all_down, index), NN)
            saved.append((hidden, normed_a, normed_m, qkv_proj, context, pre_act, hidden_mlp))
            hidden = (hidden.astype(F32) + attn_sum + bias_out[index] + mlp_sum + bias_down[index]).astype(BF16)
        y_out = gather(hidden).reshape(x_in.shape)

        grad = g_own
        wgrads = {name: [None] * n_stages for name in ('qkv', 'out', 'up', 'down')}
        vgrads = [None] * n_stages
        for index in reversed(range(n_stages)):
            hidden, normed_a, normed_m, qkv_proj, context, pre_act, hidden_mlp = saved[index]
            grad_f = grad.astype(F32)
            wgrads['down'][index] = dot(hidden_mlp, grad, TN).astype(BF16)
            grad_mlp = dot(grad, layer(all_down, index), NT)
            slope = gelu_parts(pre_act) + pre_act * jnp.exp(-0.5 * pre_act * pre_act) * ((2.0 * jnp.pi) ** -0.5)
            grad_pre = grad_mlp * slope
            grad_pre_b = grad_pre.astype(BF16)
            wgrads['up'][index] = dot(grad_pre_b, normed_m, TN).astype(BF16)
            wgrads['out'][index] = dot(context, grad, TN).astype(BF16)
            grad_context = dot(grad, layer(all_out, index), NT).astype(BF16)
            grad_qkv = attention_call(attention_backward_kernel, tabs, seq_len, 3 * width, 5, qkv_proj, grad_context)
            wgrads['qkv'][index] = dot(grad_qkv, normed_a, TN).astype(BF16)
            grad_m = dot(grad_pre_b, layer(all_up, index), NN)
            grad_a = dot(grad_qkv, layer(all_qkv, index), NN)
            normed, inv_std = normalize(hidden)
            grad_n = grad_a * gain1[index] + grad_m * gain2[index]
            mean_g = jnp.mean(grad_n, axis=-1, keepdims=True)
            mean_gn = jnp.mean(grad_n * normed, axis=-1, keepdims=True)
            vgrads[index] = (jnp.sum(grad_qkv.astype(F32), axis=0), jnp.sum(grad_pre, axis=0), jnp.sum(grad_a * normed, axis=0), jnp.sum(grad_a, axis=0), jnp.sum(grad_m * normed, axis=0), jnp.sum(grad_m, axis=0), jnp.sum(grad_f, axis=0))
            grad = (grad_f + inv_std * (grad_n - mean_g - normed * mean_gn)).astype(BF16)

        def scatter(parts):
            return lax.psum_scatter(jnp.concatenate(parts, axis=0), everyone, scatter_dimension=0, tiled=True).astype(F32)

        own = {name: scatter(parts) for name, parts in wgrads.items()}
        vec = jnp.stack([jnp.concatenate(parts) for parts in vgrads])
        vec = lax.dynamic_index_in_dim(lax.psum(vec, everyone), stage_id, 0, keepdims=False)
        sizes = [3 * width, b_up.shape[1] * tp_size] + [width] * 5
        pieces, cut = [], 0
        for size in sizes:
            pieces.append(vec[cut:cut + size])
            cut += size
        tp_rank = lax.axis_index('tp')
        d_bqkv = lax.dynamic_index_in_dim(pieces[0].reshape(tp_size, 3, heads, HEAD_DIM), tp_rank, 0, keepdims=False)
        d_bup = lax.dynamic_index_in_dim(pieces[1].reshape(tp_size, -1), tp_rank, 0, keepdims=False)
        d_qkv = jnp.transpose(own['qkv'].reshape(3, heads, HEAD_DIM, width), (3, 1, 0, 2))
        grads = (pieces[2], pieces[3], d_qkv, jnp.transpose(d_bqkv, (1, 0, 2)), own['out'].reshape(heads, HEAD_DIM, width), pieces[6], pieces[4], pieces[5], jnp.transpose(own['up']), d_bup, own['down'], pieces[6])
        return tuple([y_out] + [value[None] for value in grads])

    return jax.shard_map(device_fn, mesh=mesh, in_specs=(P('dp'), P('dp')) + STAGE_SPECS, out_specs=(P('dp'),) + GRAD_SPECS, check_vma=False)
```

```python
import jax
import jax.numpy as jnp
from jax import lax
from jax.experimental import pallas as pl
from jax.experimental.layout import Layout, with_layout_constraint
from jax.experimental.pallas import tpu as pltpu
from jax.sharding import PartitionSpec as P

ROPE_BASE = 10000.0
LN_EPS = 1e-5
HEAD_DIM = 64
STAGE_SPECS = (P('pp', None), P('pp', None), P('pp', None, 'tp', None, None), P('pp', 'tp', None, None), P('pp', 'tp', None, None), P('pp', None), P('pp', None), P('pp', None), P('pp', None, 'tp'), P('pp', 'tp'), P('pp', 'tp', None), P('pp', None))
GRAD_SPECS = (P(('dp', 'pp'), None), P(('dp', 'pp'), None), P(('dp', 'pp'), None, 'tp', None, None), P(('dp', 'pp'), 'tp', None, None), P(('dp', 'pp'), 'tp', None, None), P(('dp', 'pp'), None), P(('dp', 'pp'), None), P(('dp', 'pp'), None), P(('dp', 'pp'), None, 'tp'), P(('dp', 'pp'), 'tp'), P(('dp', 'pp'), 'tp', None), P(('dp', 'pp'), None))
F32 = jnp.float32
BF16 = jnp.bfloat16
NN = (((1,), (0,)), ((), ()))
NT = (((1,), (1,)), ((), ()))
TN = (((0,), (0,)), ((), ()))


def dot(lhs, rhs, dims):
    return lax.dot_general(lhs, rhs, dims, preferred_element_type=F32)


def rotary_lanes(seq_len):
    rot_dim = HEAD_DIM // 4
    half_rot = rot_dim // 2
    inv_freq = ROPE_BASE ** (-(jnp.arange(half_rot, dtype=F32) * 2.0) / rot_dim)
    angles = jnp.arange(seq_len, dtype=F32)[:, None] * inv_freq[None, :]
    cos, sin = jnp.cos(angles), jnp.sin(angles)
    rest = HEAD_DIM - rot_dim
    zero_half, zero_rest = jnp.zeros_like(sin), jnp.zeros((seq_len, rest), F32)
    own = jnp.concatenate([cos, cos, jnp.ones((seq_len, rest), F32)], axis=1)
    above = jnp.concatenate([-sin, zero_half, zero_rest], axis=1)
    below = jnp.concatenate([zero_half, sin, zero_rest], axis=1)
    return jnp.stack([jnp.tile(tab, (1, 2)) for tab in (own, above, below)])


def rotate(values, tabs):
    return values * tabs[0] + pltpu.roll(values, 120, 1) * tabs[1] + pltpu.roll(values, 8, 1) * tabs[2]


def rotate_back(values, tabs):
    return values * tabs[0] + pltpu.roll(values * tabs[1], 8, 1) + pltpu.roll(values * tabs[2], 120, 1)


def pair_columns(pair, half_cols):
    pairs_per_half = half_cols // 3 // 128
    base = (pair // pairs_per_half) * half_cols + (pair % pairs_per_half) * 128
    return [pl.ds(pl.multiple_of(base + part * (half_cols // 3), 128), 128) for part in range(3)]


def transposed_probs(key, query, causal):
    half = key.shape[0] // 2
    top = dot(key[:half], query, NT)
    low = dot(key[half:], query[half:], NT)
    left = jnp.where(causal, top[:, :half], -1e30)
    right = top[:, half:]
    low = jnp.where(causal, low, -1e30)
    max_left = jnp.max(left, axis=0, keepdims=True)
    max_right = jnp.maximum(jnp.max(right, axis=0, keepdims=True), jnp.max(low, axis=0, keepdims=True))
    left, right, low = jnp.exp(left - max_left), jnp.exp(right - max_right), jnp.exp(low - max_right)
    inv_left = 1.0 / jnp.sum(left, axis=0, keepdims=True)
    inv_right = 1.0 / (jnp.sum(right, axis=0, keepdims=True) + jnp.sum(low, axis=0, keepdims=True))
    return left * inv_left, right * inv_right, low * inv_right


def spread(stat_rows, top, low):
    half = low.shape[0]
    full = dot(stat_rows[:, :half], top, NN)
    return jnp.concatenate([full[:, :half], full[:, half:] + dot(stat_rows[:, half:], low, NN)], axis=1)


def attention_forward_kernel(tabs_ref, qkv_ref, ctx_ref):
    seq_len = qkv_ref.shape[0]
    half = seq_len // 2
    half_cols = qkv_ref.shape[1] // 2
    causal = lax.broadcasted_iota(jnp.int32, (half, half), 0) <= lax.broadcasted_iota(jnp.int32, (half, half), 1)
    first = lax.broadcasted_iota(jnp.int32, (seq_len, 128), 1) < HEAD_DIM
    tabs = (tabs_ref[0], tabs_ref[1], tabs_ref[2])

    @pl.loop(0, ctx_ref.shape[1] // 128, unroll=2)
    def pair_step(pair):
        q_col, k_col, v_col = pair_columns(pair, half_cols)
        query = rotate(qkv_ref[:, q_col].astype(F32), tabs).astype(BF16) * (HEAD_DIM ** -0.5)
        key = rotate(qkv_ref[:, k_col].astype(F32), tabs)
        value_t = qkv_ref[:, v_col].astype(F32).T.astype(BF16)
        outs = []
        for head, keep in enumerate((first, ~first)):
            left, right, low = transposed_probs(jnp.where(keep, key, 0.0).astype(BF16), query, causal)
            top = jnp.concatenate([left.astype(BF16), right.astype(BF16)], axis=1)
            outs.append(spread(value_t[head * HEAD_DIM:(head + 1) * HEAD_DIM], top, low.astype(BF16)))
        ctx_ref[:, pl.ds(pl.multiple_of(pair * 128, 128), 128)] = jnp.concatenate(outs, axis=0).T.astype(BF16)


def attention_backward_kernel(tabs_ref, qkv_ref, gctx_ref, gqkv_ref):
    seq_len = qkv_ref.shape[0]
    half = seq_len // 2
    half_cols = qkv_ref.shape[1] // 2
    scale = HEAD_DIM ** -0.5
    causal = lax.broadcasted_iota(jnp.int32, (half, half), 0) <= lax.broadcasted_iota(jnp.int32, (half, half), 1)
    first = lax.broadcasted_iota(jnp.int32, (seq_len, 128), 1) < HEAD_DIM
    tabs = (tabs_ref[0], tabs_ref[1], tabs_ref[2])

    @pl.loop(0, gctx_ref.shape[1] // 128)
    def pair_step(pair):
        q_col, k_col, v_col = pair_columns(pair, half_cols)
        query = rotate(qkv_ref[:, q_col].astype(F32), tabs).astype(BF16) * scale
        key32 = rotate(qkv_ref[:, k_col].astype(F32), tabs)
        key_t = key32.T.astype(BF16)
        value32 = qkv_ref[:, v_col].astype(F32)
        gctx = gctx_ref[:, pl.ds(pl.multiple_of(pair * 128, 128), 128)]
        gqueries, gkeys, gvalues = [], [], []
        for head, keep in enumerate((first, ~first)):
            value = jnp.where(keep, value32, 0.0).astype(BF16)
            left, right, low = transposed_probs(jnp.where(keep, key32, 0.0).astype(BF16), query, causal)
            gtop = dot(value[:half], gctx, NT)
            glow = dot(value[half:], gctx[half:], NT)
            gleft, gright = gtop[:, :half], gtop[:, half:]
            sum_left = jnp.sum(gleft * left, axis=0, keepdims=True)
            sum_right = jnp.sum(gright * right, axis=0, keepdims=True) + jnp.sum(glow * low, axis=0, keepdims=True)
            top = jnp.concatenate([left.astype(BF16), right.astype(BF16)], axis=1)
            low_b = low.astype(BF16)
            gvalues.append(jnp.concatenate([dot(top, gctx, NN), dot(low_b, gctx[half:], NN)], axis=0))
            dtop = jnp.concatenate([(left * (gleft - sum_left)).astype(BF16), (right * (gright - sum_right)).astype(BF16)], axis=1)
            dlow = (low * (glow - sum_right)).astype(BF16)
            gkeys.append(jnp.concatenate([dot(dtop, query, NN), dot(dlow, query[half:], NN)], axis=0))
            gqueries.append(spread(key_t[head * HEAD_DIM:(head + 1) * HEAD_DIM], dtop, dlow))
        gquery = jnp.concatenate(gqueries, axis=0).T * scale
        gqkv_ref[:, q_col] = rotate_back(gquery, tabs).astype(BF16)
        gqkv_ref[:, k_col] = rotate_back(jnp.where(first, gkeys[0], gkeys[1]), tabs).astype(BF16)
        gqkv_ref[:, v_col] = jnp.where(first, gvalues[0], gvalues[1]).astype(BF16)


def attention_call(kernel, tabs, seq_len, out_cols, n_dots, *arrays):
    tokens = arrays[0].shape[0]
    rows = tokens // seq_len
    width = arrays[0].shape[1] // 3
    heads = width // HEAD_DIM
    return pl.pallas_call(
        kernel,
        grid=(rows,),
        in_specs=[pl.BlockSpec(tabs.shape, lambda i: (0, 0, 0))] + [pl.BlockSpec((seq_len, array.shape[1]), lambda i: (i, 0)) for array in arrays],
        out_specs=pl.BlockSpec((seq_len, out_cols), lambda i: (i, 0)),
        out_shape=jax.ShapeDtypeStruct((tokens, out_cols), BF16),
        compiler_params=pltpu.CompilerParams(dimension_semantics=('arbitrary',), vmem_limit_bytes=48 * 1024 * 1024),
        cost_estimate=pl.CostEstimate(flops=2 * n_dots * rows * heads * seq_len * seq_len * 256, bytes_accessed=2 * tokens * (sum(a.shape[1] for a in arrays) + out_cols), transcendentals=rows * heads * seq_len * seq_len),
    )(tabs, *arrays)


def row_major(values):
    return with_layout_constraint(values, Layout(tuple(range(values.ndim))))


def normalize(hidden):
    hidden_f = hidden.astype(F32)
    center = hidden_f - jnp.mean(hidden_f, axis=-1, keepdims=True)
    inv_std = lax.rsqrt(jnp.mean(center * center, axis=-1, keepdims=True) + LN_EPS)
    return center * inv_std, inv_std


def gelu_parts(pre_act):
    cdf = 0.5 * (1.0 + lax.erf(pre_act * (2.0 ** -0.5)))
    return cdf


def solution(mesh):
    everyone = ('tp', 'pp')

    def device_fn(x_in, g_out, ln1_gain, ln1_bias, w_qkv, b_qkv, w_out, b_out, ln2_gain, ln2_bias, w_up, b_up, w_down, b_down):
        n_stages, tp_size = mesh.shape['pp'], mesh.shape['tp']
        n_dev = n_stages * tp_size
        stage_id = lax.axis_index('pp')
        tp_rank = lax.axis_index('tp')
        rank = tp_rank * n_stages + stage_id
        n_micro, n_rows, seq_len, width = x_in.shape
        own_micro = n_micro // n_dev
        tokens = own_micro * n_rows * seq_len
        tabs = rotary_lanes(seq_len)

        def gather(shard):
            return lax.all_gather(shard, everyone, axis=0, tiled=True)

        def exchange(rows):
            return lax.all_to_all(rows, 'pp', 0, 0, tiled=True)

        heads = w_qkv.shape[2]
        qkv_part = exchange(jnp.transpose(w_qkv[0], (2, 1, 3, 0)).reshape(3 * heads * HEAD_DIM, width))
        out_part = exchange(w_out[0].reshape(heads * HEAD_DIM, width))
        up_part = exchange(jnp.transpose(w_up[0]))
        down_part = exchange(w_down[0])

        def layer(part, index):
            rows = part.shape[0] // n_stages
            return gather(part[index * rows:(index + 1) * rows])

        weights = [tuple(layer(part, index) for part in (qkv_part, out_part, up_part, down_part)) for index in range(n_stages)]

        def small(own, columns):
            return own.reshape(1, columns).astype(F32)

        b_qkv_own = jnp.transpose(b_qkv[0], (1, 0, 2)).reshape(1, -1)
        vec_own = jnp.concatenate([small(b_qkv_own, 3 * heads * HEAD_DIM), small(b_up, b_up.shape[1]), ln1_gain, ln1_bias, ln2_gain, ln2_bias, small(b_out, width), small(b_down, width)], axis=1)
        vec_all = jnp.swapaxes(gather(vec_own).reshape(tp_size, n_stages, -1), 0, 1)
        cut = 0

        def take(columns, split):
            nonlocal cut
            part = vec_all[:, :, cut:cut + columns] if split else vec_all[:, 0, cut:cut + columns]
            cut += columns
            return part.reshape(n_stages, -1)

        bias_qkv = take(3 * heads * HEAD_DIM, True)
        bias_up = take(b_up.shape[1], True)
        gain1, shift1, gain2, shift2, bias_out, bias_down = (take(width, False) for _ in range(6))

        x_own = lax.dynamic_slice_in_dim(x_in, rank * own_micro, own_micro, 0).reshape(tokens, width)
        g_own = lax.dynamic_slice_in_dim(g_out, rank * own_micro, own_micro, 0).reshape(tokens, width).astype(BF16)

        hidden = row_major(x_own)
        saved = []
        for index in range(n_stages):
            all_qkv, all_out, all_up, all_down = weights[index]
            normed, _ = normalize(hidden)
            normed_a = (normed * gain1[index] + shift1[index]).astype(BF16)
            normed_m = (normed * gain2[index] + shift2[index]).astype(BF16)
            qkv_proj = (dot(normed_a, all_qkv, NT) + bias_qkv[index]).astype(BF16)
            context = attention_call(attention_forward_kernel, tabs, seq_len, width, 2, qkv_proj)
            attn_sum = dot(context, all_out, NN)
            pre_act = dot(normed_m, all_up, NT) + bias_up[index]
            hidden_mlp = (pre_act * gelu_parts(pre_act)).astype(BF16)
            mlp_sum = dot(hidden_mlp, all_down, NN)
            saved.append((hidden, normed_a, normed_m, qkv_proj, context, pre_act, hidden_mlp))
            hidden = row_major((hidden.astype(F32) + attn_sum + bias_out[index] + mlp_sum + bias_down[index]).astype(BF16))
        y_out = gather(hidden).reshape(x_in.shape)
        in_flight = [y_out]

        def scatter(full):
            return lax.psum_scatter(full, everyone, scatter_dimension=0, tiled=True)

        grad = row_major(g_own)
        pieces = {name: [None] * n_stages for name in ('qkv', 'out', 'up', 'down')}
        vgrads = [None] * n_stages
        for index in reversed(range(n_stages)):
            hidden, normed_a, normed_m, qkv_proj, context, pre_act, hidden_mlp = saved[index]
            all_qkv, all_out, all_up, all_down = weights[index]
            grad_f = grad.astype(F32)
            grad_context = dot(grad, all_out, NT).astype(BF16)
            grad_qkv = attention_call(attention_backward_kernel, tabs, seq_len, 3 * width, 5, qkv_proj, grad_context)
            d_out = dot(context, grad, TN).astype(BF16)
            d_qkv = dot(grad_qkv, normed_a, TN).astype(BF16)
            if index == 0:
                d_out, d_qkv, grad = lax.optimization_barrier((d_out, d_qkv, grad))
            grad_mlp = dot(grad, all_down, NT)
            slope = gelu_parts(pre_act) + pre_act * jnp.exp(-0.5 * pre_act * pre_act) * ((2.0 * jnp.pi) ** -0.5)
            grad_pre = grad_mlp * slope
            grad_pre_b = grad_pre.astype(BF16)
            d_up = dot(grad_pre_b, normed_m, TN).astype(BF16)
            if index == 0:
                d_up, grad, in_flight = lax.optimization_barrier((d_up, grad, in_flight))
            d_down = dot(hidden_mlp, grad, TN).astype(BF16)
            if index == 0:
                d_down, grad_pre_b, grad_qkv = lax.optimization_barrier((d_down, grad_pre_b, grad_qkv))
            grad_m = dot(grad_pre_b, all_up, NN)
            grad_a = dot(grad_qkv, all_qkv, NN)
            normed, inv_std = normalize(hidden)
            grad_n = grad_a * gain1[index] + grad_m * gain2[index]
            mean_g = jnp.mean(grad_n, axis=-1, keepdims=True)
            mean_gn = jnp.mean(grad_n * normed, axis=-1, keepdims=True)
            vgrads[index] = (jnp.sum(grad_qkv.astype(F32), axis=0), jnp.sum(grad_pre, axis=0), jnp.sum(grad_a * normed, axis=0), jnp.sum(grad_a, axis=0), jnp.sum(grad_m * normed, axis=0), jnp.sum(grad_m, axis=0), jnp.sum(grad_f, axis=0))
            if index > 0:
                grad = row_major((grad_f + inv_std * (grad_n - mean_g - normed * mean_gn)).astype(BF16))
                grad, d_qkv, d_out, d_up, d_down, in_flight = lax.optimization_barrier((grad, d_qkv, d_out, d_up, d_down, in_flight))
            if index < n_stages - 1:
                for name, piece in zip(('qkv', 'out', 'up', 'down'), in_flight):
                    pieces[name][index + 1] = piece
            in_flight = [scatter(full) for full in (d_qkv, d_out, d_up, d_down)]
        for name, piece in zip(('qkv', 'out', 'up', 'down'), in_flight):
            pieces[name][0] = piece

        y_out = jnp.where(stage_id < n_stages, y_out, jnp.zeros_like(y_out))
        y_out, pieces['down'][0] = lax.optimization_barrier((y_out, pieces['down'][0]))
        own = {name: exchange(jnp.concatenate(parts, axis=0)).astype(F32) for name, parts in pieces.items()}
        vec = jnp.stack([jnp.concatenate(parts) for parts in vgrads])
        vec = lax.dynamic_index_in_dim(lax.psum(vec, everyone), stage_id, 0, keepdims=False)
        sizes = [3 * width, b_up.shape[1] * tp_size] + [width] * 5
        vecs, cut = [], 0
        for size in sizes:
            vecs.append(vec[cut:cut + size])
            cut += size
        d_bqkv = lax.dynamic_index_in_dim(vecs[0].reshape(tp_size, 3, heads, HEAD_DIM), tp_rank, 0, keepdims=False)
        d_bup = lax.dynamic_index_in_dim(vecs[1].reshape(tp_size, -1), tp_rank, 0, keepdims=False)
        d_qkv = jnp.transpose(own['qkv'].reshape(3, heads, HEAD_DIM, width), (3, 1, 0, 2))
        grads = (vecs[2], vecs[3], d_qkv, jnp.transpose(d_bqkv, (1, 0, 2)), own['out'].reshape(heads, HEAD_DIM, width), vecs[6], vecs[4], vecs[5], jnp.transpose(own['up']), d_bup, own['down'], vecs[6])
        return tuple([y_out] + [value[None] for value in grads])

    return jax.shard_map(device_fn, mesh=mesh, in_specs=(P('dp'), P('dp')) + STAGE_SPECS, out_specs=(P('dp'),) + GRAD_SPECS, check_vma=False)
```

```python
import jax
import jax.numpy as jnp
from jax import lax
from jax.experimental import pallas as pl
from jax.experimental.layout import Layout, with_layout_constraint
from jax.experimental.pallas import tpu as pltpu
from jax.sharding import PartitionSpec as P

ROPE_BASE = 10000.0
LN_EPS = 1e-5
HEAD_DIM = 64
STAGE_SPECS = (P('pp', None), P('pp', None), P('pp', None, 'tp', None, None), P('pp', 'tp', None, None), P('pp', 'tp', None, None), P('pp', None), P('pp', None), P('pp', None), P('pp', None, 'tp'), P('pp', 'tp'), P('pp', 'tp', None), P('pp', None))
GRAD_SPECS = (P(('dp', 'pp'), None), P(('dp', 'pp'), None), P(('dp', 'pp'), None, 'tp', None, None), P(('dp', 'pp'), 'tp', None, None), P(('dp', 'pp'), 'tp', None, None), P(('dp', 'pp'), None), P(('dp', 'pp'), None), P(('dp', 'pp'), None), P(('dp', 'pp'), None, 'tp'), P(('dp', 'pp'), 'tp'), P(('dp', 'pp'), 'tp', None), P(('dp', 'pp'), None))
F32 = jnp.float32
BF16 = jnp.bfloat16
NN = (((1,), (0,)), ((), ()))
NT = (((1,), (1,)), ((), ()))
TN = (((0,), (0,)), ((), ()))


def dot(lhs, rhs, dims):
    return lax.dot_general(lhs, rhs, dims, preferred_element_type=F32)


def rotary_lanes(seq_len):
    rot_dim = HEAD_DIM // 4
    half_rot = rot_dim // 2
    inv_freq = ROPE_BASE ** (-(jnp.arange(half_rot, dtype=F32) * 2.0) / rot_dim)
    angles = jnp.arange(seq_len, dtype=F32)[:, None] * inv_freq[None, :]
    cos, sin = jnp.cos(angles), jnp.sin(angles)
    rest = HEAD_DIM - rot_dim
    zero_half, zero_rest = jnp.zeros_like(sin), jnp.zeros((seq_len, rest), F32)
    own = jnp.concatenate([cos, cos, jnp.ones((seq_len, rest), F32)], axis=1)
    above = jnp.concatenate([-sin, zero_half, zero_rest], axis=1)
    below = jnp.concatenate([zero_half, sin, zero_rest], axis=1)
    return jnp.stack([jnp.tile(tab, (1, 2)) for tab in (own, above, below)])


def rotate(values, tabs):
    return values * tabs[0] + pltpu.roll(values, 120, 1) * tabs[1] + pltpu.roll(values, 8, 1) * tabs[2]


def rotate_back(values, tabs):
    return values * tabs[0] + pltpu.roll(values * tabs[1], 8, 1) + pltpu.roll(values * tabs[2], 120, 1)


def pair_columns(pair, half_cols):
    pairs_per_half = half_cols // 3 // 128
    base = (pair // pairs_per_half) * half_cols + (pair % pairs_per_half) * 128
    return [pl.ds(pl.multiple_of(base + part * (half_cols // 3), 128), 128) for part in range(3)]


def transposed_probs(key, query, causal):
    half = key.shape[0] // 2
    top = dot(key[:half], query, NT)
    low = dot(key[half:], query[half:], NT)
    left = jnp.where(causal, top[:, :half], -1e30)
    right = top[:, half:]
    low = jnp.where(causal, low, -1e30)
    max_left = jnp.max(left, axis=0, keepdims=True)
    max_right = jnp.maximum(jnp.max(right, axis=0, keepdims=True), jnp.max(low, axis=0, keepdims=True))
    left, right, low = jnp.exp(left - max_left), jnp.exp(right - max_right), jnp.exp(low - max_right)
    inv_left = 1.0 / jnp.sum(left, axis=0, keepdims=True)
    inv_right = 1.0 / (jnp.sum(right, axis=0, keepdims=True) + jnp.sum(low, axis=0, keepdims=True))
    return left * inv_left, right * inv_right, low * inv_right


def spread(stat_rows, top, low):
    half = low.shape[0]
    full = dot(stat_rows[:, :half], top, NN)
    return jnp.concatenate([full[:, :half], full[:, half:] + dot(stat_rows[:, half:], low, NN)], axis=1)


def attention_forward_kernel(tabs_ref, qkv_ref, ctx_ref):
    seq_len = qkv_ref.shape[0]
    half_cols = qkv_ref.shape[1] // 2
    causal = lax.broadcasted_iota(jnp.int32, (seq_len, seq_len), 0) >= lax.broadcasted_iota(jnp.int32, (seq_len, seq_len), 1)
    first = lax.broadcasted_iota(jnp.int32, (seq_len, 128), 1) < HEAD_DIM
    tabs = (tabs_ref[0], tabs_ref[1], tabs_ref[2])

    @pl.loop(0, ctx_ref.shape[1] // 128, unroll=2)
    def pair_step(pair):
        q_col, k_col, v_col = pair_columns(pair, half_cols)
        query = rotate(qkv_ref[:, q_col].astype(F32), tabs) * (HEAD_DIM ** -0.5)
        key = rotate(qkv_ref[:, k_col].astype(F32), tabs).astype(BF16)
        value = qkv_ref[:, v_col]
        outs = []
        for keep in (first, ~first):
            scores = dot(jnp.where(keep, query, 0.0).astype(BF16), key, NT)
            scores = jnp.where(causal, scores, -1e30)
            expo = jnp.exp(scores - jnp.max(scores, axis=1, keepdims=True))
            probs = expo * (1.0 / jnp.sum(expo, axis=1, keepdims=True))
            outs.append(dot(probs.astype(BF16), value, NN))
        ctx_ref[:, pl.ds(pl.multiple_of(pair * 128, 128), 128)] = jnp.where(first, outs[0], outs[1]).astype(BF16)


def attention_backward_kernel(tabs_ref, qkv_ref, gctx_ref, gqkv_ref):
    seq_len = qkv_ref.shape[0]
    half = seq_len // 2
    half_cols = qkv_ref.shape[1] // 2
    scale = HEAD_DIM ** -0.5
    causal = lax.broadcasted_iota(jnp.int32, (half, half), 0) <= lax.broadcasted_iota(jnp.int32, (half, half), 1)
    first = lax.broadcasted_iota(jnp.int32, (seq_len, 128), 1) < HEAD_DIM
    tabs = (tabs_ref[0], tabs_ref[1], tabs_ref[2])

    @pl.loop(0, gctx_ref.shape[1] // 128)
    def pair_step(pair):
        q_col, k_col, v_col = pair_columns(pair, half_cols)
        query = rotate(qkv_ref[:, q_col].astype(F32), tabs).astype(BF16) * scale
        key32 = rotate(qkv_ref[:, k_col].astype(F32), tabs)
        key_t = key32.T.astype(BF16)
        value32 = qkv_ref[:, v_col].astype(F32)
        gctx = gctx_ref[:, pl.ds(pl.multiple_of(pair * 128, 128), 128)]
        gqueries, gkeys, gvalues = [], [], []
        for head, keep in enumerate((first, ~first)):
            value = jnp.where(keep, value32, 0.0).astype(BF16)
            left, right, low = transposed_probs(jnp.where(keep, key32, 0.0).astype(BF16), query, causal)
            gtop = dot(value[:half], gctx, NT)
            glow = dot(value[half:], gctx[half:], NT)
            gleft, gright = gtop[:, :half], gtop[:, half:]
            sum_left = jnp.sum(gleft * left, axis=0, keepdims=True)
            sum_right = jnp.sum(gright * right, axis=0, keepdims=True) + jnp.sum(glow * low, axis=0, keepdims=True)
            top = jnp.concatenate([left.astype(BF16), right.astype(BF16)], axis=1)
            low_b = low.astype(BF16)
            gvalues.append(jnp.concatenate([dot(top, gctx, NN), dot(low_b, gctx[half:], NN)], axis=0))
            dtop = jnp.concatenate([(left * (gleft - sum_left)).astype(BF16), (right * (gright - sum_right)).astype(BF16)], axis=1)
            dlow = (low * (glow - sum_right)).astype(BF16)
            gkeys.append(jnp.concatenate([dot(dtop, query, NN), dot(dlow, query[half:], NN)], axis=0))
            gqueries.append(spread(key_t[head * HEAD_DIM:(head + 1) * HEAD_DIM], dtop, dlow))
        gquery = jnp.concatenate(gqueries, axis=0).T * scale
        gqkv_ref[:, q_col] = rotate_back(gquery, tabs).astype(BF16)
        gqkv_ref[:, k_col] = rotate_back(jnp.where(first, gkeys[0], gkeys[1]), tabs).astype(BF16)
        gqkv_ref[:, v_col] = jnp.where(first, gvalues[0], gvalues[1]).astype(BF16)


def attention_call(kernel, tabs, seq_len, out_cols, n_dots, *arrays):
    tokens = arrays[0].shape[0]
    rows = tokens // seq_len
    width = arrays[0].shape[1] // 3
    heads = width // HEAD_DIM
    return pl.pallas_call(
        kernel,
        grid=(rows,),
        in_specs=[pl.BlockSpec(tabs.shape, lambda i: (0, 0, 0))] + [pl.BlockSpec((seq_len, array.shape[1]), lambda i: (i, 0)) for array in arrays],
        out_specs=pl.BlockSpec((seq_len, out_cols), lambda i: (i, 0)),
        out_shape=jax.ShapeDtypeStruct((tokens, out_cols), BF16),
        compiler_params=pltpu.CompilerParams(dimension_semantics=('arbitrary',), vmem_limit_bytes=48 * 1024 * 1024),
        cost_estimate=pl.CostEstimate(flops=2 * n_dots * rows * heads * seq_len * seq_len * 256, bytes_accessed=2 * tokens * (sum(a.shape[1] for a in arrays) + out_cols), transcendentals=rows * heads * seq_len * seq_len),
    )(tabs, *arrays)


def row_major(values):
    return with_layout_constraint(values, Layout(tuple(range(values.ndim))))


def normalize(hidden):
    hidden_f = hidden.astype(F32)
    center = hidden_f - jnp.mean(hidden_f, axis=-1, keepdims=True)
    inv_std = lax.rsqrt(jnp.mean(center * center, axis=-1, keepdims=True) + LN_EPS)
    return center * inv_std, inv_std


def gelu_parts(pre_act):
    cdf = 0.5 * (1.0 + lax.erf(pre_act * (2.0 ** -0.5)))
    return cdf


def solution(mesh):
    everyone = ('tp', 'pp')

    def device_fn(x_in, g_out, ln1_gain, ln1_bias, w_qkv, b_qkv, w_out, b_out, ln2_gain, ln2_bias, w_up, b_up, w_down, b_down):
        n_stages, tp_size = mesh.shape['pp'], mesh.shape['tp']
        n_dev = n_stages * tp_size
        stage_id = lax.axis_index('pp')
        tp_rank = lax.axis_index('tp')
        rank = tp_rank * n_stages + stage_id
        n_micro, n_rows, seq_len, width = x_in.shape
        own_micro = n_micro // n_dev
        tokens = own_micro * n_rows * seq_len
        tabs = rotary_lanes(seq_len)

        def gather(shard):
            return lax.all_gather(shard, everyone, axis=0, tiled=True)

        def exchange(rows):
            return lax.all_to_all(rows, 'pp', 0, 0, tiled=True)

        heads = w_qkv.shape[2]

        def gather_stages(shard):
            return lax.all_gather(shard, ('pp', 'tp'), axis=0, tiled=True).reshape(n_stages, -1, width)

        qkv_stages = gather_stages(jnp.transpose(w_qkv[0], (2, 1, 3, 0)).reshape(3 * heads * HEAD_DIM, width))
        out_stages = gather_stages(w_out[0].reshape(heads * HEAD_DIM, width))
        up_part = exchange(jnp.transpose(w_up[0]))

        def small(own, columns):
            return own.reshape(1, columns).astype(F32)

        b_qkv_own = jnp.transpose(b_qkv[0], (1, 0, 2)).reshape(1, -1)
        vec_own = jnp.concatenate([small(b_qkv_own, 3 * heads * HEAD_DIM), small(b_up, b_up.shape[1]), ln1_gain, ln1_bias, ln2_gain, ln2_bias, small(b_out, width), small(b_down, width)], axis=1)
        vec_all = jnp.swapaxes(gather(vec_own).reshape(tp_size, n_stages, -1), 0, 1)
        cut = 0

        def take(columns, split):
            nonlocal cut
            part = vec_all[:, :, cut:cut + columns] if split else vec_all[:, 0, cut:cut + columns]
            cut += columns
            return part.reshape(n_stages, -1)

        bias_qkv = take(3 * heads * HEAD_DIM, True)
        bias_up = take(b_up.shape[1], True)
        gain1, shift1, gain2, shift2, bias_out, bias_down = (take(width, False) for _ in range(6))

        x_own = lax.dynamic_slice_in_dim(x_in, rank * own_micro, own_micro, 0).reshape(tokens, width)
        g_own = lax.dynamic_slice_in_dim(g_out, rank * own_micro, own_micro, 0).reshape(tokens, width).astype(BF16)

        hidden = row_major(x_own)

        def normed_pair(hidden, index):
            normed, _ = normalize(hidden)
            return (normed * gain1[index] + shift1[index]).astype(BF16), (normed * gain2[index] + shift2[index]).astype(BF16)

        down_rows, tabs, normed_first, bias_qkv, bias_up = lax.optimization_barrier((w_down[0], tabs, normed_pair(hidden, 0), bias_qkv, bias_up))
        down_part = exchange(down_rows)
        qkv_stages, up_part, down_part = lax.optimization_barrier((qkv_stages, up_part, down_part))

        def layer(part, index):
            rows = part.shape[0] // n_stages
            return gather(part[index * rows:(index + 1) * rows])

        weights = [(qkv_stages[index], out_stages[index], layer(up_part, index), layer(down_part, index)) for index in range(n_stages)]

        saved = []
        for index in range(n_stages):
            all_qkv, all_out, all_up, all_down = weights[index]
            normed_a, normed_m = normed_pair(hidden, index) if index else normed_first
            qkv_proj = (dot(normed_a, all_qkv, NT) + bias_qkv[index]).astype(BF16)
            context = attention_call(attention_forward_kernel, tabs, seq_len, width, 2, qkv_proj)
            attn_sum = dot(context, all_out, NN)
            pre_act = dot(normed_m, all_up, NT) + bias_up[index]
            hidden_mlp = (pre_act * gelu_parts(pre_act)).astype(BF16)
            mlp_sum = dot(hidden_mlp, all_down, NN)
            saved.append((hidden, normed_a, normed_m, qkv_proj, context, pre_act, hidden_mlp))
            hidden = row_major((hidden.astype(F32) + attn_sum + bias_out[index] + mlp_sum + bias_down[index]).astype(BF16))
        y_out = gather(hidden).reshape(x_in.shape)
        in_flight = [y_out]

        def scatter(full):
            return lax.psum_scatter(full, everyone, scatter_dimension=0, tiled=True)

        grad = row_major(g_own)
        pieces = {name: [None] * n_stages for name in ('down', 'up', 'qkv')}
        d_outs = [None] * n_stages
        vgrads = [None] * n_stages
        for index in reversed(range(n_stages)):
            hidden, normed_a, normed_m, qkv_proj, context, pre_act, hidden_mlp = saved[index]
            all_qkv, all_out, all_up, all_down = weights[index]
            grad_f = grad.astype(F32)
            d_down = dot(hidden_mlp, grad, TN).astype(BF16)
            d_down, grad = lax.optimization_barrier((d_down, grad))
            pieces['down'][index] = scatter(d_down)
            grad_mlp = dot(grad, all_down, NT)
            slope = gelu_parts(pre_act) + pre_act * jnp.exp(-0.5 * pre_act * pre_act) * ((2.0 * jnp.pi) ** -0.5)
            grad_pre = grad_mlp * slope
            grad_pre_b = grad_pre.astype(BF16)
            d_up = dot(grad_pre_b, normed_m, TN).astype(BF16)
            d_up, grad = lax.optimization_barrier((d_up, grad))
            pieces['up'][index] = scatter(d_up)
            grad_context = dot(grad, all_out, NT).astype(BF16)
            grad_qkv = attention_call(attention_backward_kernel, tabs, seq_len, 3 * width, 5, qkv_proj, grad_context)
            d_out = dot(context, grad, TN).astype(BF16)
            d_qkv = dot(grad_qkv, normed_a, TN).astype(BF16)
            d_qkv, d_outs[index], grad_qkv, grad_pre_b, in_flight = lax.optimization_barrier((d_qkv, d_out, grad_qkv, grad_pre_b, in_flight))
            if index < n_stages - 1:
                pieces['down'][index + 1], pieces['up'][index + 1], pieces['qkv'][index + 1] = in_flight
            pieces['qkv'][index] = scatter(d_qkv)
            in_flight = [pieces[name][index] for name in ('down', 'up', 'qkv')]
            grad_m = dot(grad_pre_b, all_up, NN)
            grad_a = dot(grad_qkv, all_qkv, NN)
            normed, inv_std = normalize(hidden)
            grad_n = grad_a * gain1[index] + grad_m * gain2[index]
            mean_g = jnp.mean(grad_n, axis=-1, keepdims=True)
            mean_gn = jnp.mean(grad_n * normed, axis=-1, keepdims=True)
            vgrads[index] = (jnp.sum(grad_qkv.astype(F32), axis=0), jnp.sum(grad_pre, axis=0), jnp.sum(grad_a * normed, axis=0), jnp.sum(grad_a, axis=0), jnp.sum(grad_m * normed, axis=0), jnp.sum(grad_m, axis=0), jnp.sum(grad_f, axis=0))
            if index > 0:
                grad = row_major((grad_f + inv_std * (grad_n - mean_g - normed * mean_gn)).astype(BF16))
        own_out = lax.psum_scatter(jnp.concatenate(d_outs, axis=0), ('pp', 'tp'), scatter_dimension=0, tiled=True)

        y_out = jnp.where(stage_id < n_stages, y_out, jnp.zeros_like(y_out))
        y_out, pieces['qkv'][0] = lax.optimization_barrier((y_out, pieces['qkv'][0]))
        own = {name: exchange(jnp.concatenate(parts, axis=0)).astype(F32) for name, parts in pieces.items()}
        own['out'] = own_out.astype(F32)
        vec = jnp.sum(exchange(jnp.stack([jnp.concatenate(parts) for parts in vgrads])), axis=0)
        vec = jnp.sum(lax.all_gather(vec, 'tp', axis=0), axis=0)
        sizes = [3 * width, b_up.shape[1] * tp_size] + [width] * 5
        vecs, cut = [], 0
        for size in sizes:
            vecs.append(vec[cut:cut + size])
            cut += size
        d_bqkv = lax.dynamic_index_in_dim(vecs[0].reshape(tp_size, 3, heads, HEAD_DIM), tp_rank, 0, keepdims=False)
        d_bup = lax.dynamic_index_in_dim(vecs[1].reshape(tp_size, -1), tp_rank, 0, keepdims=False)
        d_qkv = jnp.transpose(own['qkv'].reshape(3, heads, HEAD_DIM, width), (3, 1, 0, 2))
        grads = (vecs[2], vecs[3], d_qkv, jnp.transpose(d_bqkv, (1, 0, 2)), own['out'].reshape(heads, HEAD_DIM, width), vecs[6], vecs[4], vecs[5], jnp.transpose(own['up']), d_bup, own['down'], vecs[6])
        return tuple([y_out] + [value[None] for value in grads])

    return jax.shard_map(device_fn, mesh=mesh, in_specs=(P('dp'), P('dp')) + STAGE_SPECS, out_specs=(P('dp'),) + GRAD_SPECS, check_vma=False)
```
